1024 devices in a mesh: dp: 64 (over z, x_lo, core), tensor: 16 (over y, x_hi).
Axes of the slice: x: 4 (x_hi: 2, x_lo: 2; x = x_hi * 2 + x_lo), y: 8, z: 16, core: 2. Of those that a mesh axis runs over, the one named last changes fastest.
Arguments:
- tokens: bfloat16 [32768, 2048], P(('dp', 'tensor')), may hold values from -24 to 24
- gate_weight: bfloat16 [2048, 8192], P(None, 'tensor'), may hold values from -0.125 to 0.125
- up_act: bfloat16 [32768, 8192], P('dp', 'tensor'), may hold values from -6 to 6
- cotangent: bfloat16 [32768, 8192], P('dp', 'tensor'), may hold values from -6 to 6
- moment1: bfloat16 [2048, 8192], P('dp', 'tensor'), may hold values from -0.359375 to 0.359375
- moment2: bfloat16 [2048, 8192], P('dp', 'tensor'), may hold values from 0.0039978027 to 0.039794922
Outputs:
- in_grad: bfloat16 [32768, 2048], P(('dp', 'tensor'))
- up_grad: bfloat16 [32768, 8192], P('dp', 'tensor')
- new_moment1: bfloat16 [2048, 8192], P('dp', 'tensor')
- new_moment2: bfloat16 [2048, 8192], P('dp', 'tensor')
- update: float32 [2048, 8192], P('dp', 'tensor')
The draws below stay inside these ranges and needn't reach their ends.
All inputs are finite; a program needn't handle non-finite values.
Results may differ from the reference program's by a relative error of at most 0.015.
Values may be sent and summed in bfloat16 or wider, within the bound.
A program may use at most 64 MiB of HBM per device.

```python
import math
import jax
import jax.numpy as jnp
from jax import lax

DW = 2048
FFW = 8192
GROUP = 512
REPLICAS = 64
TENSOR_WAYS = 16
TOKENS = 32768


def strengthened(array, own_key, source, target, parts, factor):
    def block_of(axis_at):
        return (jnp.arange(array.shape[axis_at]) // (array.shape[axis_at] // parts)).reshape((-1,) + (1,) * (array.ndim - 1 - axis_at))

    one_side = jax.random.permutation(own_key, parts)[block_of(target)]
    second = (block_of(target) + parts // 2) % parts
    return jnp.where((block_of(source) == one_side) | (block_of(source) == second), factor * array, array)


def block_levels(rng, shape, cuts, smallest, high):
    def one(position, blocks):
        heights = jax.random.uniform(jax.random.fold_in(jax.random.fold_in(rng, 6), position), (blocks,), jnp.float32, smallest / len(cuts), high / len(cuts))
        return jnp.repeat(jnp.exp(heights), shape[position] // blocks).reshape((-1,) + (1,) * (len(shape) - position - 1))

    factor_of = one(*cuts[0])
    for cut in cuts[1:]:
        factor_of = factor_of * one(*cut)
    return factor_of


def gaussian(stream_key, dims, deviation, most, shards=(), dtype=jnp.bfloat16):
    drawn = jax.random.normal(stream_key, dims, jnp.float32) * deviation
    if len(shards) > 0:
        drawn = block_levels(stream_key, dims, shards, -0.22, 0.18) * drawn
    return jnp.clip(drawn, min=-most, max=most).astype(dtype)


def gaussian_with(stream_key, shape, deviation, bound, shards, heavy, held_as=jnp.bfloat16):
    values = deviation * jax.random.normal(stream_key, shape, jnp.float32)
    if shards:
        values = values * block_levels(stream_key, shape, shards, -0.22, 0.18)
    return jnp.clip(strengthened(values, jax.random.fold_in(stream_key, 3), *heavy), -bound, bound).astype(held_as)


def setup_inputs(seed: int = 0) -> dict:
    keys = jax.random.split(jax.random.key(seed), 7)
    tokens = gaussian_with(keys[0], (TOKENS, DW), 1.0, 24.0, ((0, 1024),), (0, 1, 1024, 6.0))
    gate_weight = gaussian(keys[1], (DW, FFW), DW ** -0.5, 0.125, ((1, 16),))
    up_act = gaussian(keys[2], (TOKENS, FFW), 1.0, 6.0, ((0, 64), (1, 16)))
    cotangent = gaussian(keys[3], (TOKENS, FFW), 1.0, 6.0, ((0, 64), (1, 16)))
    moment1 = gaussian(keys[4], (DW, FFW), 0.06, 0.359375, ((0, 64), (1, 16)))
    moment2 = jnp.clip(jnp.exp(math.log(0.039794922) - 2.2979944 * jax.random.uniform(keys[5], (DW, FFW), jnp.float32) ** block_levels(keys[5], (DW, FFW), ((0, 64), (1, 16)), -0.2, 0.2)), 0.0039978027, 0.039794922).astype(jnp.bfloat16)
    return dict(tokens=tokens, gate_weight=gate_weight, up_act=up_act, cotangent=cotangent, moment1=moment1, moment2=moment2)


def reference(tokens, gate_weight, up_act, cotangent, moment1, moment2):
    hidden_cols = FFW // TENSOR_WAYS
    token_sets = tokens.reshape(REPLICAS, GROUP, DW)
    up_sets = up_act.reshape(REPLICAS, GROUP, FFW)
    cot_sets = cotangent.reshape(REPLICAS, GROUP, FFW)
    weight_blocks = gate_weight.astype(jnp.float32).reshape(DW, TENSOR_WAYS, hidden_cols)

    def replica(running, operands):
        feature_rows, up_rows, cot_rows = operands
        gate_pre = jnp.dot(feature_rows, gate_weight, preferred_element_type=jnp.float32)
        sigmoid_gate = jax.nn.sigmoid(gate_pre)
        cot_float = cot_rows.astype(jnp.float32)
        up_result = (cot_float * gate_pre * sigmoid_gate).astype(jnp.bfloat16)
        gate_grad = (cot_float * up_rows.astype(jnp.float32) * sigmoid_gate * (1.0 + gate_pre * (1.0 - sigmoid_gate))).astype(jnp.bfloat16)
        pieces = jnp.einsum('gkc,dkc->kgd', gate_grad.astype(jnp.float32).reshape(GROUP, TENSOR_WAYS, hidden_cols), weight_blocks)
        input_rows = lax.optimization_barrier(jnp.sum(pieces.astype(jnp.bfloat16).astype(jnp.float32), axis=0)).astype(jnp.bfloat16)
        partial_value = jnp.dot(feature_rows.T, gate_grad, preferred_element_type=jnp.float32).astype(jnp.bfloat16)
        return (running + partial_value.astype(jnp.float32), (input_rows, up_result))
    start_sum = jnp.zeros((DW, FFW), jnp.float32)
    grad_total, (input_sets, up_results) = lax.scan(replica, start_sum, (token_sets, up_sets, cot_sets))
    grad = grad_total * (1.0 / math.sqrt(REPLICAS * GROUP))
    first = 0.9 * moment1.astype(jnp.float32) + 0.1 * grad
    second = 0.95 * moment2.astype(jnp.float32) + 0.05 * grad * grad
    update = first / (jnp.sqrt(second) + 1e-08)
    return (input_sets.reshape(TOKENS, DW), up_results.reshape(TOKENS, FFW), first.astype(jnp.bfloat16), second.astype(jnp.bfloat16), update)
```

```python
import math

import jax
import jax.numpy as jnp
from jax import lax
from jax.experimental import pallas as pl
from jax.experimental.pallas import tpu as pltpu
from jax.sharding import PartitionSpec as P

F32, BF16 = jnp.float32, jnp.bfloat16
Y, Z = 8, 16
BLK = 32


def slot(dy, c):
    if dy == 0:
        return c
    if dy == Y // 2:
        return 14 + c
    return (4 * dy if dy > 0 else -4 * dy - 2) + c


def kernel(
    tok_in, wgt_in, up_in, cot_in, m1_in, m2_in,
    ig_out, upg_out, m1_out, m2_out, upd_out,
    tok, wgt, up, cot, upg, gg, term, ir_r, ir_l, xh_s, xh_r,
    w, co_r, zs, zr_r, zr_l, xl_s, xl_r, m1, m2, ig, nm1, nm2, upd,
    ld_sem, up_sem, cot_sem, st_sem, upg_sem,
    g_ss, g_rs, x_ss, x_rs, co_ss, co_rs, z_ss, z_rs, i_ss, i_rs,
):
    d = lax.axis_index("dp")
    t = lax.axis_index("tensor")
    z, x_lo, core = d // 4, (d // 2) % 2, d % 2
    y, x_hi = t // 2, t % 2
    yr = (d, (t + 2) % 16)
    yl = (d, (t + 14) % 16)
    xh = (d, t + 1 - 2 * x_hi)
    zr = ((d + 4) % 64, t)
    zl = ((d + 60) % 64, t)
    xl = (d + 2 - 4 * x_lo, t)
    co = (d + 1 - 2 * core, t)

    def remote(src, dst, ss, rs, to):
        return pltpu.make_async_remote_copy(
            src_ref=src, dst_ref=dst, send_sem=ss, recv_sem=rs,
            device_id=to, device_id_type=pl.DeviceIdType.MESH,
        )

    def rows(s, half=None):
        if half is None:
            return pl.ds(BLK * s, BLK)
        return pl.ds(BLK * s + 16 * half, 16)

    def t_of(dy, c):
        return 2 * ((y + dy + Y) % Y) + (x_hi if c == 0 else 1 - x_hi)

    places = [(dy, c) for dy in (0, -1, 1, -2, 2, -3, 3, 4) for c in (0, 1)]

    ld_tok = pltpu.make_async_copy(tok_in, tok.at[rows(0)], ld_sem.at[0])
    ld_tok.start()
    ld_wgt = pltpu.make_async_copy(wgt_in, wgt, ld_sem.at[1])
    ld_wgt.start()
    loads = {}
    for dy, c in places:
        s = slot(dy, c)
        a = pltpu.make_async_copy(up_in.at[t_of(dy, c)], up.at[rows(s)], up_sem.at[s])
        b = pltpu.make_async_copy(cot_in.at[t_of(dy, c)], cot.at[rows(s)], cot_sem.at[s])
        a.start()
        b.start()
        loads[s] = (a, b)
    ld_m1 = pltpu.make_async_copy(m1_in, m1, ld_sem.at[2])
    ld_m2 = pltpu.make_async_copy(m2_in, m2, ld_sem.at[3])
    ld_m1.start()
    ld_m2.start()

    barrier = pltpu.get_barrier_semaphore()
    for peer in (yr, yl, xh, zr, zl, xl, co):
        pl.semaphore_signal(barrier, inc=1, device_id=peer, device_id_type=pl.DeviceIdType.MESH)
    pl.semaphore_wait(barrier, 7)

    g = {}
    for h in range(1, 5):
        for c in range(2):
            hr, hl = (0, 1) if h == 4 else (None, None)
            g[0, h, c] = remote(
                tok.at[rows(slot(1 - h, c), hr)],
                tok.at[rows(slot(-h if h < 4 else 4, c), hr)],
                g_ss.at[0, h - 1, c], g_rs.at[0, h - 1, c], yr,
            )
            g[1, h, c] = remote(
                tok.at[rows(slot(h - 1, c), hl)],
                tok.at[rows(slot(h, c), hl)],
                g_ss.at[1, h - 1, c], g_rs.at[1, h - 1, c], yl,
            )
    gx = remote(tok.at[rows(0)], tok.at[rows(1)], x_ss.at[0], x_rs.at[0], xh)

    upg_st = []

    def block(first, count):
        for s in range(first, first + count):
            loads[s][0].wait()
            loads[s][1].wait()
        r = pl.ds(BLK * first, BLK * count)
        gp = jnp.dot(tok[r, :], wgt[...], preferred_element_type=F32)
        sig = 1.0 / (1.0 + jnp.exp(-gp))
        cf = cot[r, :].astype(F32)
        upg[r, :] = (cf * gp * sig).astype(BF16)
        g16 = (cf * up[r, :].astype(F32) * sig * (1.0 + gp * (1.0 - sig))).astype(BF16)
        gg[r, :] = g16
        term[r, :] = lax.dot_general(
            g16, wgt[...], (((1,), (1,)), ((), ())), preferred_element_type=F32
        ).astype(BF16)
        for dy, c in places:
            s = slot(dy, c)
            if first <= s < first + count:
                cp = pltpu.make_async_copy(upg.at[rows(s)], upg_out.at[t_of(dy, c)], upg_sem.at[s])
                cp.start()
                upg_st.append(cp)

    ld_tok.wait()
    g[0, 1, 0].start()
    g[1, 1, 0].start()
    gx.start()
    gx.wait_recv()
    g[0, 1, 1].start()
    g[1, 1, 1].start()
    ld_wgt.wait()
    block(0, 2)
    for h in range(1, 4):
        for c in range(2):
            for side in range(2):
                g[side, h, c].wait_recv()
                g[side, h + 1, c].start()
        block(4 * h - 2, 4)
    for c in range(2):
        for side in range(2):
            g[side, 4, c].wait_recv()
    block(14, 2)

    ir = (ir_r, ir_l)
    i = {}
    for s in range(1, 5):
        for u in range(2):
            for side in range(2):
                half = side if s == 1 else None
                dy = 5 - s if side == 0 or s == 1 else s - 5
                dst = ir[side].at[s - 1, u]
                if half is not None:
                    dst = ir[side].at[s - 1, u, pl.ds(16 * half, 16)]
                i[side, s, u] = remote(
                    term.at[rows(slot(dy, u), half)], dst,
                    i_ss.at[side, s - 1, u], i_rs.at[side, s - 1, u], yr if side == 0 else yl,
                )
    ix = remote(xh_s, xh_r, x_ss.at[1], x_rs.at[1], xh)

    for u in (1, 0):
        for side in range(2):
            i[side, 1, u].start()

    def i_step(k):
        s, u = (k + 1) // 2, k % 2
        for side in range(2):
            i[side, s, u].wait_recv()
            if s == 4:
                continue
            dy = 4 - s if side == 0 else s - 4
            if s == 1:
                r = rows(slot(dy, u), side)
                got = ir[side][0, u, pl.ds(16 * side, 16), :]
            else:
                r = rows(slot(dy, u))
                got = ir[side][s - 1, u]
            term[r, :] = (term[r, :].astype(F32) + got.astype(F32)).astype(BF16)
            i[side, s + 1, u].start()
        if s == 4 and u == 1:
            xh_s[...] = (
                term[rows(1), :].astype(F32) + ir_r[3, 1].astype(F32) + ir_l[3, 1].astype(F32)
            ).astype(BF16)
            ix.start()

    cos = [
        remote(w.at[k, :, 1 - core], co_r.at[k], co_ss.at[k], co_rs.at[k], co) for k in range(Z)
    ]

    def w_part(dzs):
        for dz in dzs:
            k = dz % Z
            zt = (z + dz + Z) % Z
            cols = tok[:, pl.ds(pl.multiple_of(zt * 128, 128), 128)]
            part = lax.dot_general(
                cols, gg[...], (((0,), (0,)), ((), ())), preferred_element_type=F32
            )
            w[k] = part.astype(BF16).reshape(2, 2, BLK, part.shape[-1])
            cos[k].start()

    zrv = (zr_r, zr_l)
    zc = {}
    for s in range(1, 9):
        for side in range(2):
            for q in range(2):
                if s == 1 and q != side:
                    continue
                k = (9 - s if side == 0 else s - 9) % Z
                zc[side, s, q] = remote(
                    zs.at[k, q], zrv[side].at[s - 1, q],
                    z_ss.at[side, s - 1, q], z_rs.at[side, s - 1, q], zr if side == 0 else zl,
                )

    def own(k, q):
        return w[k, q, core].astype(F32) + co_r[k, q].astype(F32)

    def z_step(s):
        for side in range(2):
            cos[(8 - s if side == 0 else s - 8) % Z].wait_recv()
        for q in range(2):
            for side in range(2):
                k = (8 - s if side == 0 else s - 8) % Z
                val = own(k, q)
                if s > 1 or q == side:
                    zc[side, s, q].wait_recv()
                    val = val + zrv[side][s - 1, q].astype(F32)
                zs[k, q] = val.astype(BF16)
                zc[side, s + 1, q].start()

    w_part([8])
    w_part([7, -7])
    cos[8].wait_recv()
    for q in range(2):
        zs[8, q] = own(8, q).astype(BF16)
        zc[q, 1, q].start()
    w_part([6, -6])
    for k in range(1, 8):
        z_step(k)
        if k < 6:
            w_part([6 - k, k - 6])
        elif k == 6:
            w_part([0])
        i_step(k)

    cos[0].wait_recv()
    for q in range(2):
        for side in range(2):
            zc[side, 8, q].wait_recv()

    def total(q):
        return (
            w[0, q, core].astype(F32) + co_r[0, q].astype(F32)
            + zr_r[7, q].astype(F32) + zr_l[7, q].astype(F32)
        )

    xl_s[...] = total(1 - x_lo).astype(BF16)
    xc = remote(xl_s, xl_r, x_ss.at[2], x_rs.at[2], xl)
    xc.start()
    i_step(8)
    ld_m1.wait()
    ld_m2.wait()
    mine = total(x_lo)
    xc.wait_recv()
    grad = (mine + xl_r[...].astype(F32)) * (1.0 / math.sqrt(32768))
    first = 0.9 * m1[...].astype(F32) + 0.1 * grad
    second = 0.95 * m2[...].astype(F32) + 0.05 * grad * grad
    upd[...] = first / (jnp.sqrt(second) + 1e-8)
    nm1[...] = first.astype(BF16)
    nm2[...] = second.astype(BF16)
    stores = [
        pltpu.make_async_copy(upd, upd_out, st_sem.at[0]),
        pltpu.make_async_copy(nm1, m1_out, st_sem.at[1]),
        pltpu.make_async_copy(nm2, m2_out, st_sem.at[2]),
    ]
    for st in stores:
        st.start()
    ix.wait_recv()
    ig[...] = (
        term[rows(0), :].astype(F32) + ir_r[3, 0].astype(F32) + ir_l[3, 0].astype(F32)
        + xh_r[...].astype(F32)
    ).astype(BF16)
    stores.append(pltpu.make_async_copy(ig, ig_out, st_sem.at[3]))
    stores[-1].start()

    gx.wait_send()
    ix.wait_send()
    xc.wait_send()
    for cp in [*g.values(), *i.values(), *cos, *zc.values()]:
        cp.wait_send()
    for st in [*upg_st, *stores]:
        st.wait()


def local(tokens, gate_weight, up_act, cotangent, moment1, moment2):
    dw, hid = gate_weight.shape
    any_spec = pl.BlockSpec(memory_space=pl.ANY)
    vm = pltpu.VMEM
    dma = pltpu.SemaphoreType.DMA
    ig, upg, nm1, nm2, upd = pl.pallas_call(
        kernel,
        out_shape=(
            jax.ShapeDtypeStruct((BLK, dw), BF16),
            jax.ShapeDtypeStruct((16, BLK, hid), BF16),
            jax.ShapeDtypeStruct((BLK, hid), BF16),
            jax.ShapeDtypeStruct((BLK, hid), BF16),
            jax.ShapeDtypeStruct((BLK, hid), F32),
        ),
        in_specs=[any_spec] * 6,
        out_specs=(any_spec,) * 5,
        scratch_shapes=[
            vm((512, dw), BF16),
            vm((dw, hid), BF16),
            vm((512, hid), BF16),
            vm((512, hid), BF16),
            vm((512, hid), BF16),
            vm((512, hid), BF16),
            vm((512, dw), BF16),
            vm((4, 2, BLK, dw), BF16),
            vm((4, 2, BLK, dw), BF16),
            vm((BLK, dw), BF16),
            vm((BLK, dw), BF16),
            vm((Z, 2, 2, BLK, hid), BF16),
            vm((Z, 2, BLK, hid), BF16),
            vm((Z, 2, BLK, hid), BF16),
            vm((8, 2, BLK, hid), BF16),
            vm((8, 2, BLK, hid), BF16),
            vm((BLK, hid), BF16),
            vm((BLK, hid), BF16),
            vm((BLK, hid), BF16),
            vm((BLK, hid), BF16),
            vm((BLK, dw), BF16),
            vm((BLK, hid), BF16),
            vm((BLK, hid), BF16),
            vm((BLK, hid), F32),
            dma((4,)), dma((16,)), dma((16,)), dma((4,)), dma((16,)),
            dma((2, 4, 2)), dma((2, 4, 2)), dma((3,)), dma((3,)),
            dma((Z,)), dma((Z,)), dma((2, 8, 2)), dma((2, 8, 2)),
            dma((2, 4, 2)), dma((2, 4, 2)),
        ],
        compiler_params=pltpu.CompilerParams(collective_id=0, has_side_effects=True),
    )(
        tokens,
        gate_weight,
        up_act.reshape(16, BLK, hid),
        cotangent.reshape(16, BLK, hid),
        moment1,
        moment2,
    )
    return ig, upg.reshape(512, hid), nm1, nm2, upd


def solution(mesh):
    rows, cols, both = P(("dp", "tensor"), None), P(None, "tensor"), P("dp", "tensor")
    return jax.shard_map(
        local,
        mesh=mesh,
        in_specs=(rows, cols, both, both, both, both),
        out_specs=(rows, both, both, both, both),
        check_vma=False,
    )
```

```python
import math

import jax
import jax.numpy as jnp
from jax import lax
from jax.experimental import pallas as pl
from jax.experimental.pallas import tpu as pltpu
from jax.sharding import PartitionSpec as P

F32, BF16 = jnp.float32, jnp.bfloat16
Y, Z = 8, 16
BLK = 32


def slot(dy, c):
    if dy == 0:
        return c
    if dy == Y // 2:
        return 14 + c
    return (4 * dy if dy > 0 else -4 * dy - 2) + c


def kernel(
    tok_in, wgt_in, up_in, cot_in,
    upg_out, ig, grad,
    tok, wgt, up, cot, upg, gg, term, ir_r, ir_l, xh_s, xh_r,
    w, co_r, zs, zr_r, zr_l, xl_s, xl_r,
    ld_sem, up_sem, cot_sem, upg_sem,
    g_ss, g_rs, gx_ss, gx_rs, x_ss, x_rs, co_ss, co_rs, z_ss, z_rs, i_ss, i_rs,
):
    d = lax.axis_index("dp")
    t = lax.axis_index("tensor")
    z, x_lo, core = d // 4, (d // 2) % 2, d % 2
    y, x_hi = t // 2, t % 2
    yn = ((d, (t + 2) % 16), (d, (t + 14) % 16))
    xh = (d, t + 1 - 2 * x_hi)
    zn = (((d + 4) % 64, t), ((d + 60) % 64, t))
    zn2 = (((d + 8) % 64, t), ((d + 56) % 64, t))
    xl = (d + 2 - 4 * x_lo, t)
    co = (d + 1 - 2 * core, t)

    def remote(src, dst, ss, rs, to):
        return pltpu.make_async_remote_copy(
            src_ref=src, dst_ref=dst, send_sem=ss, recv_sem=rs,
            device_id=to, device_id_type=pl.DeviceIdType.MESH,
        )

    def rows(s, half=None):
        if half is None:
            return pl.ds(BLK * s, BLK)
        return pl.ds(BLK * s + 16 * half, 16)

    def t_of(dy, c):
        return 2 * ((y + dy + Y) % Y) + (x_hi if c == 0 else 1 - x_hi)

    places = [(dy, c) for dy in (0, -1, 1, -2, 2, -3, 3, 4) for c in (0, 1)]

    ld_tok = pltpu.make_async_copy(tok_in, tok.at[rows(0)], ld_sem.at[0])
    ld_tok.start()
    ld_wgt = pltpu.make_async_copy(wgt_in, wgt, ld_sem.at[1])
    ld_wgt.start()
    loads = {}
    for dy, c in places:
        s = slot(dy, c)
        a = pltpu.make_async_copy(up_in.at[t_of(dy, c)], up.at[rows(s)], up_sem.at[s])
        b = pltpu.make_async_copy(cot_in.at[t_of(dy, c)], cot.at[rows(s)], cot_sem.at[s])
        a.start()
        b.start()
        loads[s] = (a, b)

    barrier = pltpu.get_barrier_semaphore()
    for peer in (*yn, xh, *zn, *zn2, xl, co):
        pl.semaphore_signal(barrier, inc=1, device_id=peer, device_id_type=pl.DeviceIdType.MESH)
    pl.semaphore_wait(barrier, 9)

    g = {}
    units = ((0, 1), (0, 0), (1, 0))
    for side in range(2):
        sg = -1 if side == 0 else 1
        for h in range(1, 5):
            for n, (c, half) in enumerate(units):
                if h == 4 and (n == 0) == (side == 0):
                    continue
                g[side, h, n] = remote(
                    tok.at[rows(slot(sg * (h - 1), c), half)],
                    tok.at[rows(slot(sg * h if h < 4 else 4, c), half)],
                    g_ss.at[side, h - 1, n], g_rs.at[side, h - 1, n], yn[side],
                )
    xa = remote(tok.at[rows(0, 0)], tok.at[rows(1, 0)], gx_ss.at[8], gx_rs.at[8], xh)
    xb = {
        dy: remote(
            tok.at[rows(slot(dy, 0), 1)], tok.at[rows(slot(dy, 1), 1)],
            gx_ss.at[dy + 3], gx_rs.at[dy + 3], xh,
        )
        for dy in (0, -1, 1, -2, 2, -3, 3, 4)
    }

    upg_st = []

    def gate(first, count):
        for s in range(first, first + count):
            loads[s][0].wait()
            loads[s][1].wait()
        r = pl.ds(BLK * first, BLK * count)
        gp = jnp.dot(tok[r, :], wgt[...], preferred_element_type=F32)
        sig = 1.0 / (1.0 + jnp.exp(-gp))
        cf = cot[r, :].astype(F32)
        upg[r, :] = (cf * gp * sig).astype(BF16)
        gg[r, :] = (cf * up[r, :].astype(F32) * sig * (1.0 + gp * (1.0 - sig))).astype(BF16)

    def terms(first, count):
        r = pl.ds(BLK * first, BLK * count)
        term[r, :] = lax.dot_general(
            gg[r, :], wgt[...], (((1,), (1,)), ((), ())), preferred_element_type=F32
        ).astype(BF16)
        for dy, c in places:
            s = slot(dy, c)
            if first <= s < first + count:
                cp = pltpu.make_async_copy(upg.at[rows(s)], upg_out.at[t_of(dy, c)], upg_sem.at[s])
                cp.start()
                upg_st.append(cp)

    ld_tok.wait()
    for n in range(2):
        for side in range(2):
            g[side, 1, n].start()
    xa.start()
    xb[0].start()
    xa.wait_recv()
    for side in range(2):
        g[side, 1, 2].start()
    ld_wgt.wait()
    for h in range(1, 4):
        for n in range(3):
            for side in range(2):
                g[side, h, n].wait_recv()
                if (side, h + 1, n) in g:
                    g[side, h + 1, n].start()
                if n == 0:
                    xb[-h if side == 0 else h].start()
            if n == 1 and h > 1:
                if h == 2:
                    xb[0].wait_recv()
                    gate(0, 2)
                    terms(0, 2)
                else:
                    xb[1 - h].wait_recv()
                    xb[h - 1].wait_recv()
                    gate(4 * h - 6, 4)
                    terms(4 * h - 6, 4)
        if h == 2:
            xb[-1].wait_recv()
            xb[1].wait_recv()
            gate(2, 4)
            terms(2, 4)
    g[1, 4, 0].wait_recv()
    xb[4].start()
    xb[-3].wait_recv()
    xb[3].wait_recv()
    gate(10, 4)
    terms(10, 4)
    g[0, 4, 1].wait_recv()
    g[0, 4, 2].wait_recv()
    xb[4].wait_recv()
    gate(14, 2)

    ir = (ir_r, ir_l)
    i = {}
    for s in range(1, 5):
        for u in range(2):
            for side in range(2):
                half = side if s == 1 else None
                dy = 5 - s if side == 0 or s == 1 else s - 5
                dst = ir[side].at[s - 1, u]
                if half is not None:
                    dst = ir[side].at[s - 1, u, pl.ds(16 * half, 16)]
                i[side, s, u] = remote(
                    term.at[rows(slot(dy, u), half)], dst,
                    i_ss.at[side, s - 1, u], i_rs.at[side, s - 1, u], yn[side],
                )
    ix = remote(xh_s, xh_r, x_ss.at[0], x_rs.at[0], xh)

    def i_step(k):
        s, u = (k + 1) // 2, k % 2
        for side in range(2):
            i[side, s, u].wait_recv()
            if s == 4:
                continue
            dy = 4 - s if side == 0 else s - 4
            if s == 1:
                r = rows(slot(dy, u), side)
                got = ir[side][0, u, pl.ds(16 * side, 16), :]
            else:
                r = rows(slot(dy, u))
                got = ir[side][s - 1, u]
            term[r, :] = (term[r, :].astype(F32) + got.astype(F32)).astype(BF16)
            i[side, s + 1, u].start()
        if s == 4 and u == 1:
            xh_s[...] = (
                term[rows(1), :].astype(F32) + ir_r[3, 1].astype(F32) + ir_l[3, 1].astype(F32)
            ).astype(BF16)
            ix.start()

    cos = [
        remote(w.at[k, :, 1 - core], co_r.at[k], co_ss.at[k], co_rs.at[k], co) for k in range(Z)
    ]

    def w_part(*dzs):
        cols = [
            tok[:, pl.ds(pl.multiple_of(((z + dz + Z) % Z) * 128, 128), 128)] for dz in dzs
        ]
        cols = cols[0] if len(cols) == 1 else jnp.concatenate(cols, axis=1)
        part = lax.dot_general(
            cols, gg[...], (((0,), (0,)), ((), ())), preferred_element_type=F32
        ).astype(BF16)
        for n, dz in enumerate(dzs):
            w[dz % Z] = part[128 * n : 128 * (n + 1)].reshape(2, 2, BLK, part.shape[-1])
            cos[dz % Z].start()

    zrv = (zr_r, zr_l)
    zc = {}
    for side in range(2):
        for k in range(1, 9):
            for q in range(2):
                if k == 8 and q != side:
                    continue
                to = zn2 if k in (7, 5, 3) else zn
                zc[side, k, q] = remote(
                    zs.at[(k if side == 0 else -k) % Z, q], zrv[side].at[k - 1, q],
                    z_ss.at[side, k - 1, q], z_rs.at[side, k - 1, q], to[side],
                )

    def z_send(k):
        for side in range(2):
            if k < 8 or side == 0:
                cos[(k if side == 0 else -k) % Z].wait_recv()
        for q in range(2):
            for side in range(2):
                if k == 8 and q != side:
                    continue
                kk = (k if side == 0 else -k) % Z
                val = w[kk, q, core].astype(F32) + co_r[kk, q].astype(F32)
                if k % 2:
                    for src in (k + 1, k + 2):
                        if (side, src, q) in zc:
                            if src == 8 or src < 8 and (src % 2 == 0 or src in (7, 5, 3)):
                                zc[side, src, q].wait_recv()
                                val = val + zrv[side][src - 1, q].astype(F32)
                zs[kk, q] = val.astype(BF16)
                zc[side, k, q].start()

    w_part(8)
    terms(14, 2)
    for u in (1, 0):
        for side in range(2):
            i[side, 1, u].start()
    w_part(7, -7)
    z_send(8)
    w_part(6, -6)
    w_part(5, -5)
    z_send(6)
    z_send(7)
    w_part(4, -4)
    w_part(3, -3)
    z_send(4)
    i_step(1)
    i_step(2)
    z_send(5)
    w_part(2, -2)
    w_part(1, -1)
    z_send(2)
    i_step(3)
    i_step(4)
    z_send(3)
    w_part(0)
    i_step(5)
    i_step(6)
    z_send(1)
    i_step(7)

    cos[0].wait_recv()
    for q in range(2):
        for side in range(2):
            zc[side, 1, q].wait_recv()

    def total(q):
        return (
            w[0, q, core].astype(F32) + co_r[0, q].astype(F32)
            + zr_r[0, q].astype(F32) + zr_l[0, q].astype(F32)
        )

    xl_s[...] = total(1 - x_lo).astype(BF16)
    xc = remote(xl_s, xl_r, x_ss.at[1], x_rs.at[1], xl)
    xc.start()
    i_step(8)
    mine = total(x_lo)
    xc.wait_recv()
    grad[...] = mine + xl_r[...].astype(F32)
    ix.wait_recv()
    ig[...] = (
        term[rows(0), :].astype(F32) + ir_r[3, 0].astype(F32) + ir_l[3, 0].astype(F32)
        + xh_r[...].astype(F32)
    ).astype(BF16)

    for cp in [xa, *xb.values(), ix, xc, *g.values(), *i.values(), *cos, *zc.values()]:
        cp.wait_send()
    for st in upg_st:
        st.wait()


def finish(ig_in, upg_in, grad_in, m1_in, m2_in, ig, upg, m1, m2, upd):
    grad = grad_in[...] * (1.0 / math.sqrt(32768))
    first = 0.9 * m1_in[...].astype(F32) + 0.1 * grad
    second = 0.95 * m2_in[...].astype(F32) + 0.05 * grad * grad
    upd[...] = first / (jnp.sqrt(second) + 1e-8)
    m1[...] = first.astype(BF16)
    m2[...] = second.astype(BF16)
    ig[...] = ig_in[...]
    upg[...] = upg_in[...]


def local(tokens, gate_weight, up_act, cotangent, moment1, moment2):
    dw, hid = gate_weight.shape
    any_spec = pl.BlockSpec(memory_space=pl.ANY)
    vm_spec = pl.BlockSpec(memory_space=pltpu.VMEM)
    vm = pltpu.VMEM
    dma = pltpu.SemaphoreType.DMA
    upg, ig, grad = pl.pallas_call(
        kernel,
        out_shape=(
            jax.ShapeDtypeStruct((16, BLK, hid), BF16),
            jax.ShapeDtypeStruct((BLK, dw), BF16),
            jax.ShapeDtypeStruct((BLK, hid), F32),
        ),
        in_specs=[any_spec] * 4,
        out_specs=(any_spec, vm_spec, vm_spec),
        scratch_shapes=[
            vm((512, dw), BF16),
            vm((dw, hid), BF16),
            vm((512, hid), BF16),
            vm((512, hid), BF16),
            vm((512, hid), BF16),
            vm((512, hid), BF16),
            vm((512, dw), BF16),
            vm((4, 2, BLK, dw), BF16),
            vm((4, 2, BLK, dw), BF16),
            vm((BLK, dw), BF16),
            vm((BLK, dw), BF16),
            vm((Z, 2, 2, BLK, hid), BF16),
            vm((Z, 2, BLK, hid), BF16),
            vm((Z, 2, BLK, hid), BF16),
            vm((8, 2, BLK, hid), BF16),
            vm((8, 2, BLK, hid), BF16),
            vm((BLK, hid), BF16),
            vm((BLK, hid), BF16),
            dma((2,)), dma((16,)), dma((16,)), dma((16,)),
            dma((2, 4, 3)), dma((2, 4, 3)), dma((9,)), dma((9,)), dma((2,)), dma((2,)),
            dma((Z,)), dma((Z,)), dma((2, 8, 2)), dma((2, 8, 2)),
            dma((2, 4, 2)), dma((2, 4, 2)),
        ],
        compiler_params=pltpu.CompilerParams(collective_id=0, has_side_effects=True),
    )(tokens, gate_weight, up_act.reshape(16, BLK, hid), cotangent.reshape(16, BLK, hid))
    return pl.pallas_call(
        finish,
        out_shape=(
            jax.ShapeDtypeStruct((BLK, dw), BF16),
            jax.ShapeDtypeStruct((512, hid), BF16),
            jax.ShapeDtypeStruct((BLK, hid), BF16),
            jax.ShapeDtypeStruct((BLK, hid), BF16),
            jax.ShapeDtypeStruct((BLK, hid), F32),
        ),
        in_specs=[vm_spec] * 5,
        out_specs=(vm_spec,) * 5,
    )(ig, upg.reshape(512, hid), grad, moment1, moment2)


def solution(mesh):
    rows, cols, both = P(("dp", "tensor"), None), P(None, "tensor"), P("dp", "tensor")
    return jax.shard_map(
        local,
        mesh=mesh,
        in_specs=(rows, cols, both, both, both, both),
        out_specs=(rows, both, both, both, both),
        check_vma=False,
    )
```

```python
import math

import jax
import jax.numpy as jnp
from jax import lax
from jax.experimental import pallas as pl
from jax.experimental.pallas import tpu as pltpu
from jax.sharding import PartitionSpec as P

F32, BF16 = jnp.float32, jnp.bfloat16
Y, Z = 8, 16
BLK = 32
HOPS = {8: 6, 7: 6, 5: 3, 4: 3, 6: 3, 2: 0, 1: 0, 3: 0}


def slot(dy, c):
    if dy == 0:
        return c
    if dy == Y // 2:
        return 14 + c
    return (4 * dy if dy > 0 else -4 * dy - 2) + c


def kernel(
    tok_in, wgt_in, up_in, cot_in,
    upg_out, ig, grad,
    tok, wgt, up, cot, upg, gg, term, ir_r, ir_l, xh_s, xh_r,
    w, co_r, zs, zr_r, zr_l, xl_s, xl_r,
    ld_sem, up_sem, cot_sem, upg_sem,
    g_ss, g_rs, gx_ss, gx_rs, x_ss, x_rs, xc_ss, xc_rs, co_ss, co_rs, z_ss, z_rs, i_ss, i_rs,
):
    d = lax.axis_index("dp")
    t = lax.axis_index("tensor")
    z, x_lo, core = d // 4, (d // 2) % 2, d % 2
    y, x_hi = t // 2, t % 2
    yn = ((d, (t + 2) % 16), (d, (t + 14) % 16))
    xh = (d, t + 1 - 2 * x_hi)
    zn = {n: (((d + 4 * n) % 64, t), ((d + 64 - 4 * n) % 64, t)) for n in (1, 2, 3)}
    xl = (d + 2 - 4 * x_lo, t)
    co = (d + 1 - 2 * core, t)

    def remote(src, dst, ss, rs, to):
        return pltpu.make_async_remote_copy(
            src_ref=src, dst_ref=dst, send_sem=ss, recv_sem=rs,
            device_id=to, device_id_type=pl.DeviceIdType.MESH,
        )

    def rows(s, half=None):
        if half is None:
            return pl.ds(BLK * s, BLK)
        return pl.ds(BLK * s + 16 * half, 16)

    def t_of(dy, c):
        return 2 * ((y + dy + Y) % Y) + (x_hi if c == 0 else 1 - x_hi)

    places = [(dy, c) for dy in (0, -1, 1, -2, 2, -3, 3, 4) for c in (0, 1)]

    ld_tok = pltpu.make_async_copy(tok_in, tok.at[rows(0)], ld_sem.at[0])
    ld_tok.start()
    ld_wgt = pltpu.make_async_copy(wgt_in, wgt, ld_sem.at[1])
    ld_wgt.start()
    loads = {}
    for dy, c in places:
        s = slot(dy, c)
        a = pltpu.make_async_copy(up_in.at[t_of(dy, c)], up.at[rows(s)], up_sem.at[s])
        b = pltpu.make_async_copy(cot_in.at[t_of(dy, c)], cot.at[rows(s)], cot_sem.at[s])
        a.start()
        b.start()
        loads[s] = (a, b)

    barrier = pltpu.get_barrier_semaphore()
    for peer in (*yn, xh, *zn[1], *zn[2], *zn[3], xl, co):
        pl.semaphore_signal(barrier, inc=1, device_id=peer, device_id_type=pl.DeviceIdType.MESH)
    pl.semaphore_wait(barrier, 11)

    g = {}
    units = ((0, 1), (0, 0), (1, 0))
    for side in range(2):
        sg = -1 if side == 0 else 1
        for h in range(1, 5):
            for n, (c, half) in enumerate(units):
                if h == 4 and (n == 0) == (side == 0):
                    continue
                g[side, h, n] = remote(
                    tok.at[rows(slot(sg * (h - 1), c), half)],
                    tok.at[rows(slot(sg * h if h < 4 else 4, c), half)],
                    g_ss.at[side, h - 1, n], g_rs.at[side, h - 1, n], yn[side],
                )
    xa = remote(tok.at[rows(0, 0)], tok.at[rows(1, 0)], gx_ss.at[8], gx_rs.at[8], xh)
    xb = {
        dy: remote(
            tok.at[rows(slot(dy, 0), 1)], tok.at[rows(slot(dy, 1), 1)],
            gx_ss.at[dy + 3], gx_rs.at[dy + 3], xh,
        )
        for dy in (0, -1, 1, -2, 2, -3, 3, 4)
    }

    upg_st = []

    def gate(first, count):
        for s in range(first, first + count):
            loads[s][0].wait()
            loads[s][1].wait()
        r = pl.ds(BLK * first, BLK * count)
        gp = jnp.dot(tok[r, :], wgt[...], preferred_element_type=F32)
        sig = 1.0 / (1.0 + jnp.exp(-gp))
        cf = cot[r, :].astype(F32)
        upg[r, :] = (cf * gp * sig).astype(BF16)
        gg[r, :] = (cf * up[r, :].astype(F32) * sig * (1.0 + gp * (1.0 - sig))).astype(BF16)

    def terms(first, count):
        r = pl.ds(BLK * first, BLK * count)
        term[r, :] = lax.dot_general(
            gg[r, :], wgt[...], (((1,), (1,)), ((), ())), preferred_element_type=F32
        ).astype(BF16)
        for dy, c in places:
            s = slot(dy, c)
            if first <= s < first + count:
                cp = pltpu.make_async_copy(upg.at[rows(s)], upg_out.at[t_of(dy, c)], upg_sem.at[s])
                cp.start()
                upg_st.append(cp)

    ld_tok.wait()
    for n in range(2):
        for side in range(2):
            g[side, 1, n].start()
    xa.start()
    xb[0].start()
    xa.wait_recv()
    for side in range(2):
        g[side, 1, 2].start()
    ld_wgt.wait()
    for h in range(1, 4):
        for n in range(3):
            for side in range(2):
                g[side, h, n].wait_recv()
                if (side, h + 1, n) in g:
                    g[side, h + 1, n].start()
                if n == 0:
                    xb[-h if side == 0 else h].start()
            if n == 1 and h > 1:
                if h == 2:
                    xb[0].wait_recv()
                    gate(0, 2)
                    terms(0, 2)
                else:
                    xb[1 - h].wait_recv()
                    xb[h - 1].wait_recv()
                    gate(4 * h - 6, 4)
                    terms(4 * h - 6, 4)
        if h == 2:
            xb[-1].wait_recv()
            xb[1].wait_recv()
            gate(2, 4)
            terms(2, 4)
    g[1, 4, 0].wait_recv()
    xb[4].start()
    xb[-3].wait_recv()
    xb[3].wait_recv()
    gate(10, 4)
    terms(10, 4)
    g[0, 4, 1].wait_recv()
    g[0, 4, 2].wait_recv()
    xb[4].wait_recv()
    gate(14, 2)

    ir = (ir_r, ir_l)
    i = {}
    for s in range(1, 5):
        for u in range(2):
            for side in range(2):
                half = side if s == 1 else None
                dy = 5 - s if side == 0 or s == 1 else s - 5
                dst = ir[side].at[s - 1, u]
                if half is not None:
                    dst = ir[side].at[s - 1, u, pl.ds(16 * half, 16)]
                i[side, s, u] = remote(
                    term.at[rows(slot(dy, u), half)], dst,
                    i_ss.at[side, s - 1, u], i_rs.at[side, s - 1, u], yn[side],
                )
    ix = remote(xh_s, xh_r, x_ss, x_rs, xh)

    def i_step(k):
        s, u = (k + 1) // 2, k % 2
        for side in range(2):
            i[side, s, u].wait_recv()
            if s == 4:
                continue
            dy = 4 - s if side == 0 else s - 4
            if s == 1:
                r = rows(slot(dy, u), side)
                got = ir[side][0, u, pl.ds(16 * side, 16), :]
            else:
                r = rows(slot(dy, u))
                got = ir[side][s - 1, u]
            term[r, :] = (term[r, :].astype(F32) + got.astype(F32)).astype(BF16)
            i[side, s + 1, u].start()
        if s == 4 and u == 1:
            xh_s[...] = (
                term[rows(1), :].astype(F32) + ir_r[3, 1].astype(F32) + ir_l[3, 1].astype(F32)
            ).astype(BF16)
            ix.start()

    cos = [
        remote(w.at[k, :, 1 - core], co_r.at[k], co_ss.at[k], co_rs.at[k], co) for k in range(Z)
    ]

    def w_part(*dzs):
        cols = [
            tok[:, pl.ds(pl.multiple_of(((z + dz + Z) % Z) * 128, 128), 128)] for dz in dzs
        ]
        cols = cols[0] if len(cols) == 1 else jnp.concatenate(cols, axis=1)
        part = lax.dot_general(
            cols, gg[...], (((0,), (0,)), ((), ())), preferred_element_type=F32
        ).astype(BF16)
        for n, dz in enumerate(dzs):
            w[dz % Z] = part[128 * n : 128 * (n + 1)].reshape(2, 2, BLK, part.shape[-1])
            cos[dz % Z].start()

    zrv = (zr_r, zr_l)
    xc = [remote(xl_s.at[k], xl_r.at[k], xc_ss.at[k], xc_rs.at[k], xl) for k in range(Z)]
    zc = {}
    for side in range(2):
        for k, to in HOPS.items():
            for q in range(2):
                if k == 8 and q != side:
                    continue
                zc[side, k, q] = remote(
                    zs.at[(k if side == 0 else -k) % Z, q], zrv[side].at[k - 1, q],
                    z_ss.at[side, k - 1, q], z_rs.at[side, k - 1, q], zn[k - to][side],
                )

    def x_send(*dzs):
        for dz in dzs:
            k = dz % Z
            cos[k].wait_recv()
            xl_s[k] = (
                w[k, 1 - x_lo, core].astype(F32) + co_r[k, 1 - x_lo].astype(F32)
            ).astype(BF16)
            xc[k].start()

    def own(k, q):
        r = pl.ds(16 * q, 16)
        return (
            w[k, x_lo, core, r, :].astype(F32) + co_r[k, x_lo, r, :].astype(F32)
            + xl_r[k, r, :].astype(F32)
        )

    def z_send(k):
        for side in range(2):
            if k < 8 or side == 0:
                xc[(k if side == 0 else -k) % Z].wait_recv()
        for q in range(2):
            for side in range(2):
                if k == 8 and q != side:
                    continue
                kk = (k if side == 0 else -k) % Z
                val = own(kk, q)
                for src, to in HOPS.items():
                    if to == k and (side, src, q) in zc:
                        zc[side, src, q].wait_recv()
                        val = val + zrv[side][src - 1, q].astype(F32)
                zs[kk, q] = val.astype(BF16)
                zc[side, k, q].start()

    w_part(8)
    terms(14, 2)
    for u in (1, 0):
        for side in range(2):
            i[side, 1, u].start()
    w_part(7, -7)
    x_send(8)
    w_part(5, -5)
    x_send(7, -7)
    w_part(4, -4)
    x_send(5, -5)
    w_part(6, -6)
    x_send(4, -4)
    w_part(2, -2)
    x_send(6, -6)
    z_send(8)
    w_part(1, -1)
    x_send(2, -2)
    z_send(7)
    i_step(1)
    w_part(3, -3)
    x_send(1, -1)
    i_step(2)
    z_send(5)
    w_part(0)
    x_send(3, -3)
    z_send(4)
    x_send(0)
    z_send(6)
    i_step(3)
    z_send(2)
    z_send(1)
    i_step(4)
    z_send(3)
    i_step(5)
    i_step(6)
    i_step(7)

    xc[0].wait_recv()
    for q in range(2):
        val = own(0, q)
        for k in (1, 2, 3):
            for side in range(2):
                zc[side, k, q].wait_recv()
                val = val + zrv[side][k - 1, q].astype(F32)
        grad[pl.ds(16 * q, 16), :] = val
    i_step(8)
    ix.wait_recv()
    ig[...] = (
        term[rows(0), :].astype(F32) + ir_r[3, 0].astype(F32) + ir_l[3, 0].astype(F32)
        + xh_r[...].astype(F32)
    ).astype(BF16)

    for cp in [xa, *xb.values(), ix, *xc, *g.values(), *i.values(), *cos, *zc.values()]:
        cp.wait_send()
    for st in upg_st:
        st.wait()


def finish(ig_in, upg_in, grad_in, m1_in, m2_in, ig, upg, m1, m2, upd):
    grad = grad_in[...] * (1.0 / math.sqrt(32768))
    first = 0.9 * m1_in[...].astype(F32) + 0.1 * grad
    second = 0.95 * m2_in[...].astype(F32) + 0.05 * grad * grad
    upd[...] = first / (jnp.sqrt(second) + 1e-8)
    m1[...] = first.astype(BF16)
    m2[...] = second.astype(BF16)
    ig[...] = ig_in[...]
    upg[...] = upg_in[...]


def local(tokens, gate_weight, up_act, cotangent, moment1, moment2):
    dw, hid = gate_weight.shape
    any_spec = pl.BlockSpec(memory_space=pl.ANY)
    vm_spec = pl.BlockSpec(memory_space=pltpu.VMEM)
    vm = pltpu.VMEM
    dma = pltpu.SemaphoreType.DMA
    upg, ig, grad = pl.pallas_call(
        kernel,
        out_shape=(
            jax.ShapeDtypeStruct((16, BLK, hid), BF16),
            jax.ShapeDtypeStruct((BLK, dw), BF16),
            jax.ShapeDtypeStruct((BLK, hid), F32),
        ),
        in_specs=[any_spec] * 4,
        out_specs=(any_spec, vm_spec, vm_spec),
        scratch_shapes=[
            vm((512, dw), BF16),
            vm((dw, hid), BF16),
            vm((512, hid), BF16),
            vm((512, hid), BF16),
            vm((512, hid), BF16),
            vm((512, hid), BF16),
            vm((512, dw), BF16),
            vm((4, 2, BLK, dw), BF16),
            vm((4, 2, BLK, dw), BF16),
            vm((BLK, dw), BF16),
            vm((BLK, dw), BF16),
            vm((Z, 2, 2, BLK, hid), BF16),
            vm((Z, 2, BLK, hid), BF16),
            vm((Z, 2, 16, hid), BF16),
            vm((8, 2, 16, hid), BF16),
            vm((8, 2, 16, hid), BF16),
            vm((Z, BLK, hid), BF16),
            vm((Z, BLK, hid), BF16),
            dma((2,)), dma((16,)), dma((16,)), dma((16,)),
            dma((2, 4, 3)), dma((2, 4, 3)), dma((9,)), dma((9,)), dma, dma, dma((Z,)), dma((Z,)),
            dma((Z,)), dma((Z,)), dma((2, 8, 2)), dma((2, 8, 2)),
            dma((2, 4, 2)), dma((2, 4, 2)),
        ],
        compiler_params=pltpu.CompilerParams(collective_id=0, has_side_effects=True),
    )(tokens, gate_weight, up_act.reshape(16, BLK, hid), cotangent.reshape(16, BLK, hid))
    return pl.pallas_call(
        finish,
        out_shape=(
            jax.ShapeDtypeStruct((BLK, dw), BF16),
            jax.ShapeDtypeStruct((512, hid), BF16),
            jax.ShapeDtypeStruct((BLK, hid), BF16),
            jax.ShapeDtypeStruct((BLK, hid), BF16),
            jax.ShapeDtypeStruct((BLK, hid), F32),
        ),
        in_specs=[vm_spec] * 5,
        out_specs=(vm_spec,) * 5,
    )(ig, upg.reshape(512, hid), grad, moment1, moment2)


def solution(mesh):
    rows, cols, both = P(("dp", "tensor"), None), P(None, "tensor"), P("dp", "tensor")
    return jax.shard_map(
        local,
        mesh=mesh,
        in_specs=(rows, cols, both, both, both, both),
        out_specs=(rows, both, both, both, both),
        check_vma=False,
    )
```

```python
import math

import jax
import jax.numpy as jnp
from jax import lax
from jax.experimental import pallas as pl
from jax.experimental.pallas import tpu as pltpu
from jax.sharding import PartitionSpec as P

F32, BF16 = jnp.float32, jnp.bfloat16
Y, Z = 8, 16
BLK = 32
HOPS = {8: 6, 7: 6, 5: 3, 4: 3, 6: 3, 2: 0, 1: 0, 3: 0}


def slot(dy, c):
    if dy == 0:
        return c
    if dy == Y // 2:
        return 14 + c
    return (4 * dy if dy > 0 else -4 * dy - 2) + c


def kernel(
    tok_in, wgt_in, up_in, cot_in,
    upg_out, ig, grad,
    tok, wgt, up, cot, upg, gg, term, ir_r, ir_l, xh_s, xh_r, pm_r,
    w, co_r, zs, zr_r, zr_l, xl_s, xl_r,
    ld_sem, up_sem, cot_sem, upg_sem,
    g_ss, g_rs, gx_ss, gx_rs, x_ss, x_rs, xc_ss, xc_rs, pm_ss, pm_rs, co_ss, co_rs, z_ss, z_rs, i_ss, i_rs,
):
    d = lax.axis_index("dp")
    t = lax.axis_index("tensor")
    z, x_lo, core = d // 4, (d // 2) % 2, d % 2
    y, x_hi = t // 2, t % 2
    yn = ((d, (t + 2) % 16), (d, (t + 14) % 16))
    xh = (d, t + 1 - 2 * x_hi)
    zn = {n: (((d + 4 * n) % 64, t), ((d + 64 - 4 * n) % 64, t)) for n in (1, 2, 3)}
    xl = (d + 2 - 4 * x_lo, t)
    co = (d + 1 - 2 * core, t)

    def remote(src, dst, ss, rs, to):
        return pltpu.make_async_remote_copy(
            src_ref=src, dst_ref=dst, send_sem=ss, recv_sem=rs,
            device_id=to, device_id_type=pl.DeviceIdType.MESH,
        )

    def rows(s, half=None):
        if half is None:
            return pl.ds(BLK * s, BLK)
        return pl.ds(BLK * s + 16 * half, 16)

    def t_of(dy, c):
        return 2 * ((y + dy + Y) % Y) + (x_hi if c == 0 else 1 - x_hi)

    places = [(dy, c) for dy in (0, -1, 1, -2, 2, -3, 3, 4) for c in (0, 1)]

    ld_tok = pltpu.make_async_copy(tok_in, tok.at[rows(0)], ld_sem.at[0])
    ld_tok.start()
    ld_wgt = pltpu.make_async_copy(wgt_in, wgt, ld_sem.at[1])
    ld_wgt.start()
    loads = {}
    for dy, c in places:
        s = slot(dy, c)
        a = pltpu.make_async_copy(up_in.at[t_of(dy, c)], up.at[rows(s)], up_sem.at[s])
        b = pltpu.make_async_copy(cot_in.at[t_of(dy, c)], cot.at[rows(s)], cot_sem.at[s])
        a.start()
        b.start()
        loads[s] = (a, b)

    barrier = pltpu.get_barrier_semaphore()
    for peer in (*yn, xh, *zn[1], *zn[2], *zn[3], xl, co):
        pl.semaphore_signal(barrier, inc=1, device_id=peer, device_id_type=pl.DeviceIdType.MESH)
    pl.semaphore_wait(barrier, 11)

    g = {}
    units = ((0, 1), (0, 0), (1, 0))
    for side in range(2):
        sg = -1 if side == 0 else 1
        for h in range(1, 5):
            for n, (c, half) in enumerate(units):
                if h == 4 and (n == 0) == (side == 0):
                    continue
                g[side, h, n] = remote(
                    tok.at[rows(slot(sg * (h - 1), c), half)],
                    tok.at[rows(slot(sg * h if h < 4 else 4, c), half)],
                    g_ss.at[side, h - 1, n], g_rs.at[side, h - 1, n], yn[side],
                )
    xa = remote(tok.at[rows(0, 0)], tok.at[rows(1, 0)], gx_ss.at[8], gx_rs.at[8], xh)
    xb = {
        dy: remote(
            tok.at[rows(slot(dy, 0), 1)], tok.at[rows(slot(dy, 1), 1)],
            gx_ss.at[dy + 3], gx_rs.at[dy + 3], xh,
        )
        for dy in (0, -1, 1, -2, 2, -3, 3, 4)
    }

    pm = {
        dy: remote(
            term.at[rows(slot(dy, 1), int(dy > 0))], pm_r.at[dy + 3],
            pm_ss.at[dy + 3], pm_rs.at[dy + 3], xh,
        )
        for dy in (-1, 1, -2, 2, -3, 3)
    }
    upg_st = []

    def gate(first, count):
        for s in range(first, first + count):
            loads[s][0].wait()
            loads[s][1].wait()
        r = pl.ds(BLK * first, BLK * count)
        gp = jnp.dot(tok[r, :], wgt[...], preferred_element_type=F32)
        sig = 1.0 / (1.0 + jnp.exp(-gp))
        cf = cot[r, :].astype(F32)
        upg[r, :] = (cf * gp * sig).astype(BF16)
        gg[r, :] = (cf * up[r, :].astype(F32) * sig * (1.0 + gp * (1.0 - sig))).astype(BF16)

    def terms(first, count):
        r = pl.ds(BLK * first, BLK * count)
        term[r, :] = lax.dot_general(
            gg[r, :], wgt[...], (((1,), (1,)), ((), ())), preferred_element_type=F32
        ).astype(BF16)
        for dy, c in places:
            s = slot(dy, c)
            if first <= s < first + count:
                cp = pltpu.make_async_copy(upg.at[rows(s)], upg_out.at[t_of(dy, c)], upg_sem.at[s])
                cp.start()
                upg_st.append(cp)

    ld_tok.wait()
    for n in range(2):
        for side in range(2):
            g[side, 1, n].start()
    xa.start()
    xb[0].start()
    xa.wait_recv()
    for side in range(2):
        g[side, 1, 2].start()
    ld_wgt.wait()
    for h in range(1, 4):
        for n in range(3):
            for side in range(2):
                g[side, h, n].wait_recv()
                if (side, h + 1, n) in g:
                    g[side, h + 1, n].start()
                if n == 0:
                    xb[-h if side == 0 else h].start()
            if n == 1 and h > 1:
                if h == 2:
                    xb[0].wait_recv()
                    gate(0, 2)
                    terms(0, 2)
                else:
                    xb[1 - h].wait_recv()
                    xb[h - 1].wait_recv()
                    gate(4 * h - 6, 4)
                    terms(4 * h - 6, 4)
        if h == 2:
            xb[-1].wait_recv()
            xb[1].wait_recv()
            gate(2, 4)
            terms(2, 4)
    g[1, 4, 0].wait_recv()
    xb[4].start()
    xb[-3].wait_recv()
    xb[3].wait_recv()
    gate(10, 4)
    terms(10, 4)
    pm[3].start()
    pm[-3].start()
    g[0, 4, 1].wait_recv()
    g[0, 4, 2].wait_recv()
    xb[4].wait_recv()
    gate(14, 2)

    ir = (ir_r, ir_l)
    i = {}
    for s in range(1, 5):
        for u in range(2):
            for side in range(2):
                half = side if s == 1 or u == 1 else None
                dy = 5 - s if side == 0 or s == 1 else s - 5
                dst = ir[side].at[s - 1, u]
                if half is not None:
                    dst = ir[side].at[s - 1, u, pl.ds(16 * half, 16)]
                i[side, s, u] = remote(
                    term.at[rows(slot(dy, u), half)], dst,
                    i_ss.at[side, s - 1, u], i_rs.at[side, s - 1, u], yn[side],
                )
    ix = remote(xh_s, xh_r, x_ss, x_rs, xh)

    def i_step(k):
        s, u = (k + 1) // 2, k % 2
        for side in range(2):
            i[side, s, u].wait_recv()
            if s == 4:
                continue
            dy = 4 - s if side == 0 else s - 4
            mine, rest = pl.ds(16 * side, 16), pl.ds(16 - 16 * side, 16)
            r = rows(slot(dy, u), side)
            term[r, :] = (
                term[r, :].astype(F32) + ir[side][s - 1, u, mine, :].astype(F32)
            ).astype(BF16)
            if u == 0:
                r = rows(slot(dy, 0), 1 - side)
                pm[dy].wait_recv()
                val = term[r, :].astype(F32) + pm_r[dy + 3].astype(F32)
                if s > 1:
                    val = val + ir[side][s - 1, 0, rest, :].astype(F32)
                term[r, :] = val.astype(BF16)
            i[side, s + 1, u].start()
        if s == 4 and u == 1:
            for side in range(2):
                half = pl.ds(16 * side, 16)
                xh_s[half, :] = (
                    term[rows(1, side), :].astype(F32) + ir[side][3, 1, half, :].astype(F32)
                ).astype(BF16)
            ix.start()

    cos = [
        remote(w.at[k, :, 1 - core], co_r.at[k], co_ss.at[k], co_rs.at[k], co) for k in range(Z)
    ]

    def w_part(*dzs):
        cols = [
            tok[:, pl.ds(pl.multiple_of(((z + dz + Z) % Z) * 128, 128), 128)] for dz in dzs
        ]
        cols = cols[0] if len(cols) == 1 else jnp.concatenate(cols, axis=1)
        part = lax.dot_general(
            cols, gg[...], (((0,), (0,)), ((), ())), preferred_element_type=F32
        ).astype(BF16)
        for n, dz in enumerate(dzs):
            w[dz % Z] = part[128 * n : 128 * (n + 1)].reshape(2, 2, BLK, part.shape[-1])
            cos[dz % Z].start()

    zrv = (zr_r, zr_l)
    xc = [remote(xl_s.at[k], xl_r.at[k], xc_ss.at[k], xc_rs.at[k], xl) for k in range(Z)]
    zc = {}
    for side in range(2):
        for k, to in HOPS.items():
            for q in range(2):
                if k == 8 and q != side:
                    continue
                zc[side, k, q] = remote(
                    zs.at[(k if side == 0 else -k) % Z, q], zrv[side].at[k - 1, q],
                    z_ss.at[side, k - 1, q], z_rs.at[side, k - 1, q], zn[k - to][side],
                )

    def x_send(*dzs):
        for dz in dzs:
            k = dz % Z
            cos[k].wait_recv()
            xl_s[k] = (
                w[k, 1 - x_lo, core].astype(F32) + co_r[k, 1 - x_lo].astype(F32)
            ).astype(BF16)
            xc[k].start()

    def own(k, q):
        r = pl.ds(16 * q, 16)
        return (
            w[k, x_lo, core, r, :].astype(F32) + co_r[k, x_lo, r, :].astype(F32)
            + xl_r[k, r, :].astype(F32)
        )

    def z_send(k):
        for side in range(2):
            if k < 8 or side == 0:
                xc[(k if side == 0 else -k) % Z].wait_recv()
        for q in range(2):
            for side in range(2):
                if k == 8 and q != side:
                    continue
                kk = (k if side == 0 else -k) % Z
                val = own(kk, q)
                for src, to in HOPS.items():
                    if to == k and (side, src, q) in zc:
                        zc[side, src, q].wait_recv()
                        val = val + zrv[side][src - 1, q].astype(F32)
                zs[kk, q] = val.astype(BF16)
                zc[side, k, q].start()

    w_part(8)
    terms(14, 2)
    for u in (1, 0):
        for side in range(2):
            i[side, 1, u].start()
    w_part(7, -7)
    x_send(8)
    w_part(5, -5)
    x_send(7, -7)
    pm[2].start()
    pm[-2].start()
    w_part(4, -4)
    x_send(5, -5)
    w_part(6, -6)
    x_send(4, -4)
    w_part(2, -2)
    x_send(6, -6)
    pm[1].start()
    pm[-1].start()
    z_send(8)
    w_part(1, -1)
    x_send(2, -2)
    z_send(7)
    i_step(1)
    w_part(3, -3)
    x_send(1, -1)
    i_step(2)
    z_send(5)
    w_part(0)
    x_send(3, -3)
    z_send(4)
    x_send(0)
    z_send(6)
    i_step(3)
    z_send(2)
    z_send(1)
    i_step(4)
    z_send(3)
    i_step(5)
    i_step(6)
    i_step(7)

    xc[0].wait_recv()
    for q in range(2):
        val = own(0, q)
        for k in (1, 2, 3):
            for side in range(2):
                zc[side, k, q].wait_recv()
                val = val + zrv[side][k - 1, q].astype(F32)
        grad[pl.ds(16 * q, 16), :] = val
    i_step(8)
    ix.wait_recv()
    ig[...] = (
        term[rows(0), :].astype(F32) + ir_r[3, 0].astype(F32) + ir_l[3, 0].astype(F32)
        + xh_r[...].astype(F32)
    ).astype(BF16)

    for cp in [xa, *xb.values(), *pm.values(), ix, *xc, *g.values(), *i.values(), *cos, *zc.values()]:
        cp.wait_send()
    for st in upg_st:
        st.wait()


def finish(
    ig_in, upg_in, grad_in, m1_in, m2_in, ig_out, upg_out, m1_out, m2_out, upd_out,
    ig, upg, grad_v, m1, m2, nm1, nm2, upd, in_sem, out_sem,
):
    ins, bufs = (grad_in, m1_in, m2_in, upg_in, ig_in), (grad_v, m1, m2, upg, ig)
    gets = [pltpu.make_async_copy(a, b, in_sem.at[n]) for n, (a, b) in enumerate(zip(ins, bufs))]
    for get in gets:
        get.start()
    outs = ((upd, upd_out), (nm1, m1_out), (nm2, m2_out), (upg, upg_out), (ig, ig_out))
    puts = [pltpu.make_async_copy(a, b, out_sem.at[n]) for n, (a, b) in enumerate(outs)]
    for n in (0, 1, 2):
        gets[n].wait()
    grad = grad_v[...] * (1.0 / math.sqrt(32768))
    first = 0.9 * m1[...].astype(F32) + 0.1 * grad
    second = 0.95 * m2[...].astype(F32) + 0.05 * grad * grad
    upd[...] = first / (jnp.sqrt(second) + 1e-8)
    nm1[...] = first.astype(BF16)
    nm2[...] = second.astype(BF16)
    for n in (3, 4):
        gets[n].wait()
        puts[n].start()
    for n in (0, 1, 2):
        puts[n].start()
    for put in puts:
        put.wait()


def local(tokens, gate_weight, up_act, cotangent, moment1, moment2):
    dw, hid = gate_weight.shape
    any_spec = pl.BlockSpec(memory_space=pl.ANY)
    vm_spec = pl.BlockSpec(memory_space=pltpu.VMEM)
    vm = pltpu.VMEM
    dma = pltpu.SemaphoreType.DMA
    upg, ig, grad = pl.pallas_call(
        kernel,
        out_shape=(
            jax.ShapeDtypeStruct((16, BLK, hid), BF16),
            jax.ShapeDtypeStruct((BLK, dw), BF16),
            jax.ShapeDtypeStruct((BLK, hid), F32),
        ),
        in_specs=[any_spec] * 4,
        out_specs=(any_spec, vm_spec, vm_spec),
        scratch_shapes=[
            vm((512, dw), BF16),
            vm((dw, hid), BF16),
            vm((512, hid), BF16),
            vm((512, hid), BF16),
            vm((512, hid), BF16),
            vm((512, hid), BF16),
            vm((512, dw), BF16),
            vm((4, 2, BLK, dw), BF16),
            vm((4, 2, BLK, dw), BF16),
            vm((BLK, dw), BF16),
            vm((BLK, dw), BF16),
            vm((7, 16, dw), BF16),
            vm((Z, 2, 2, BLK, hid), BF16),
            vm((Z, 2, BLK, hid), BF16),
            vm((Z, 2, 16, hid), BF16),
            vm((8, 2, 16, hid), BF16),
            vm((8, 2, 16, hid), BF16),
            vm((Z, BLK, hid), BF16),
            vm((Z, BLK, hid), BF16),
            dma((2,)), dma((16,)), dma((16,)), dma((16,)),
            dma((2, 4, 3)), dma((2, 4, 3)), dma((9,)), dma((9,)), dma, dma, dma((Z,)), dma((Z,)), dma((7,)), dma((7,)),
            dma((Z,)), dma((Z,)), dma((2, 8, 2)), dma((2, 8, 2)),
            dma((2, 4, 2)), dma((2, 4, 2)),
        ],
        compiler_params=pltpu.CompilerParams(collective_id=0, has_side_effects=True),
    )(tokens, gate_weight, up_act.reshape(16, BLK, hid), cotangent.reshape(16, BLK, hid))
    return pl.pallas_call(
        finish,
        out_shape=(
            jax.ShapeDtypeStruct((BLK, dw), BF16),
            jax.ShapeDtypeStruct((512, hid), BF16),
            jax.ShapeDtypeStruct((BLK, hid), BF16),
            jax.ShapeDtypeStruct((BLK, hid), BF16),
            jax.ShapeDtypeStruct((BLK, hid), F32),
        ),
        in_specs=[any_spec] * 5,
        out_specs=(any_spec,) * 5,
        scratch_shapes=[
            vm((BLK, dw), BF16), vm((512, hid), BF16), vm((BLK, hid), F32),
            vm((BLK, hid), BF16), vm((BLK, hid), BF16), vm((BLK, hid), BF16),
            vm((BLK, hid), BF16), vm((BLK, hid), F32), dma((5,)), dma((5,)),
        ],
    )(ig, upg.reshape(512, hid), grad, moment1, moment2)


def solution(mesh):
    rows, cols, both = P(("dp", "tensor"), None), P(None, "tensor"), P("dp", "tensor")
    return jax.shard_map(
        local,
        mesh=mesh,
        in_specs=(rows, cols, both, both, both, both),
        out_specs=(rows, both, both, both, both),
        check_vma=False,
    )
```

```python
import math

import jax
import jax.numpy as jnp
from jax import lax
from jax.experimental import pallas as pl
from jax.experimental.pallas import tpu as pltpu
from jax.sharding import PartitionSpec as P

F32, BF16 = jnp.float32, jnp.bfloat16
Y, Z = 8, 16
BLK = 32
HOPS = {8: 6, 7: 6, 5: 3, 4: 3, 6: 3, 2: 0, 1: 0, 3: 0}


def slot(dy, c):
    if dy == 0:
        return c
    if dy == Y // 2:
        return 14 + c
    return (4 * dy if dy > 0 else -4 * dy - 2) + c


def kernel(
    tok_in, wgt_in, up_in, cot_in,
    upg_out, ig, grad,
    tok, wgt, up, cot, upg, gg, term, ir_r, ir_l, xh_s, xh_r,
    w, co_r, zs, zr_r, zr_l, xl_s, xl_r,
    ld_sem, up_sem, cot_sem, upg_sem,
    g_ss, g_rs, gx_ss, gx_rs, x_ss, x_rs, xc_ss, xc_rs, co_ss, co_rs, z_ss, z_rs, i_ss, i_rs,
):
    d = lax.axis_index("dp")
    t = lax.axis_index("tensor")
    z, x_lo, core = d // 4, (d // 2) % 2, d % 2
    y, x_hi = t // 2, t % 2
    yn = ((d, (t + 2) % 16), (d, (t + 14) % 16))
    xh = (d, t + 1 - 2 * x_hi)
    zn = {n: (((d + 4 * n) % 64, t), ((d + 64 - 4 * n) % 64, t)) for n in (1, 2, 3)}
    xl = (d + 2 - 4 * x_lo, t)
    co = (d + 1 - 2 * core, t)

    def remote(src, dst, ss, rs, to):
        return pltpu.make_async_remote_copy(
            src_ref=src, dst_ref=dst, send_sem=ss, recv_sem=rs,
            device_id=to, device_id_type=pl.DeviceIdType.MESH,
        )

    def rows(s, half=None):
        if half is None:
            return pl.ds(BLK * s, BLK)
        return pl.ds(BLK * s + 16 * half, 16)

    def t_of(dy, c):
        return 2 * ((y + dy + Y) % Y) + (x_hi if c == 0 else 1 - x_hi)

    places = [(dy, c) for dy in (0, -1, 1, -2, 2, -3, 3, 4) for c in (0, 1)]

    ld_tok = pltpu.make_async_copy(tok_in, tok.at[rows(0)], ld_sem.at[0])
    ld_tok.start()
    ld_wgt = pltpu.make_async_copy(wgt_in, wgt, ld_sem.at[1])
    ld_wgt.start()
    loads = {}
    for dy, c in places:
        s = slot(dy, c)
        a = pltpu.make_async_copy(up_in.at[t_of(dy, c)], up.at[rows(s)], up_sem.at[s])
        b = pltpu.make_async_copy(cot_in.at[t_of(dy, c)], cot.at[rows(s)], cot_sem.at[s])
        a.start()
        b.start()
        loads[s] = (a, b)

    barrier = pltpu.get_barrier_semaphore()
    for peer in (*yn, xh, *zn[1], *zn[2], *zn[3], xl, co):
        pl.semaphore_signal(barrier, inc=1, device_id=peer, device_id_type=pl.DeviceIdType.MESH)
    pl.semaphore_wait(barrier, 11)

    g = {}
    units = ((0, 1), (0, 0), (1, 0))
    for side in range(2):
        sg = -1 if side == 0 else 1
        for h in range(1, 5):
            for n, (c, half) in enumerate(units):
                if h == 4 and (n == 0) == (side == 0):
                    continue
                g[side, h, n] = remote(
                    tok.at[rows(slot(sg * (h - 1), c), half)],
                    tok.at[rows(slot(sg * h if h < 4 else 4, c), half)],
                    g_ss.at[side, h - 1, n], g_rs.at[side, h - 1, n], yn[side],
                )
    xa = remote(tok.at[rows(0, 0)], tok.at[rows(1, 0)], gx_ss.at[8], gx_rs.at[8], xh)
    xb = {
        dy: remote(
            tok.at[rows(slot(dy, 0), 1)], tok.at[rows(slot(dy, 1), 1)],
            gx_ss.at[dy + 3], gx_rs.at[dy + 3], xh,
        )
        for dy in (0, -1, 1, -2, 2, -3, 3, 4)
    }

    upg_st = []

    def gate(first, count):
        for s in range(first, first + count):
            loads[s][0].wait()
            loads[s][1].wait()
        r = pl.ds(BLK * first, BLK * count)
        gp = jnp.dot(tok[r, :], wgt[...], preferred_element_type=F32)
        sig = 1.0 / (1.0 + jnp.exp(-gp))
        cf = cot[r, :].astype(F32)
        upg[r, :] = (cf * gp * sig).astype(BF16)
        gg[r, :] = (cf * up[r, :].astype(F32) * sig * (1.0 + gp * (1.0 - sig))).astype(BF16)

    def terms(first, count):
        r = pl.ds(BLK * first, BLK * count)
        term[r, :] = lax.dot_general(
            gg[r, :], wgt[...], (((1,), (1,)), ((), ())), preferred_element_type=F32
        ).astype(BF16)
        for dy, c in places:
            s = slot(dy, c)
            if first <= s < first + count:
                cp = pltpu.make_async_copy(upg.at[rows(s)], upg_out.at[t_of(dy, c)], upg_sem.at[s])
                cp.start()
                upg_st.append(cp)

    ld_tok.wait()
    for n in range(2):
        for side in range(2):
            g[side, 1, n].start()
    xa.start()
    xb[0].start()
    xa.wait_recv()
    for side in range(2):
        g[side, 1, 2].start()
    ld_wgt.wait()
    for h in range(1, 4):
        for n in range(3):
            for side in range(2):
                g[side, h, n].wait_recv()
                if (side, h + 1, n) in g:
                    g[side, h + 1, n].start()
                if n == 0:
                    xb[-h if side == 0 else h].start()
            if n == 1 and h > 1:
                if h == 2:
                    xb[0].wait_recv()
                    gate(0, 2)
                    terms(0, 2)
                else:
                    xb[1 - h].wait_recv()
                    xb[h - 1].wait_recv()
                    gate(4 * h - 6, 4)
                    terms(4 * h - 6, 4)
        if h == 2:
            xb[-1].wait_recv()
            xb[1].wait_recv()
            gate(2, 4)
            terms(2, 4)
    g[1, 4, 0].wait_recv()
    xb[4].start()
    xb[-3].wait_recv()
    xb[3].wait_recv()
    gate(10, 4)
    terms(10, 4)
    g[0, 4, 1].wait_recv()
    g[0, 4, 2].wait_recv()
    xb[4].wait_recv()
    gate(14, 2)

    ir = (ir_r, ir_l)
    i = {}
    for s in range(1, 5):
        for u in range(2):
            for side in range(2):
                half = side if s == 1 else None
                dy = 5 - s if side == 0 or s == 1 else s - 5
                dst = ir[side].at[s - 1, u]
                if half is not None:
                    dst = ir[side].at[s - 1, u, pl.ds(16 * half, 16)]
                i[side, s, u] = remote(
                    term.at[rows(slot(dy, u), half)], dst,
                    i_ss.at[side, s - 1, u], i_rs.at[side, s - 1, u], yn[side],
                )
    ix = remote(xh_s, xh_r, x_ss, x_rs, xh)

    def i_step(k):
        s, u = (k + 1) // 2, k % 2
        for side in range(2):
            i[side, s, u].wait_recv()
            if s == 4:
                continue
            dy = 4 - s if side == 0 else s - 4
            if s == 1:
                r = rows(slot(dy, u), side)
                got = ir[side][0, u, pl.ds(16 * side, 16), :]
            else:
                r = rows(slot(dy, u))
                got = ir[side][s - 1, u]
            term[r, :] = (term[r, :].astype(F32) + got.astype(F32)).astype(BF16)
            i[side, s + 1, u].start()
        if s == 4 and u == 1:
            xh_s[...] = (
                term[rows(1), :].astype(F32) + ir_r[3, 1].astype(F32) + ir_l[3, 1].astype(F32)
            ).astype(BF16)
            ix.start()

    cos = [
        remote(w.at[k, :, 1 - core], co_r.at[k], co_ss.at[k], co_rs.at[k], co) for k in range(Z)
    ]

    def w_part(*dzs):
        cols = [
            tok[:, pl.ds(pl.multiple_of(((z + dz + Z) % Z) * 128, 128), 128)] for dz in dzs
        ]
        cols = cols[0] if len(cols) == 1 else jnp.concatenate(cols, axis=1)
        part = lax.dot_general(
            cols, gg[...], (((0,), (0,)), ((), ())), preferred_element_type=F32
        ).astype(BF16)
        for n, dz in enumerate(dzs):
            w[dz % Z] = part[128 * n : 128 * (n + 1)].reshape(2, 2, BLK, part.shape[-1])
            cos[dz % Z].start()

    zrv = (zr_r, zr_l)
    xc = [remote(xl_s.at[k], xl_r.at[k], xc_ss.at[k], xc_rs.at[k], xl) for k in range(Z)]
    zc = {}
    for side in range(2):
        for k, to in HOPS.items():
            for q in range(2):
                if k == 8 and q != side:
                    continue
                zc[side, k, q] = remote(
                    zs.at[(k if side == 0 else -k) % Z, q], zrv[side].at[k - 1, q],
                    z_ss.at[side, k - 1, q], z_rs.at[side, k - 1, q], zn[k - to][side],
                )

    def x_send(*dzs):
        for dz in dzs:
            k = dz % Z
            cos[k].wait_recv()
            xl_s[k] = (
                w[k, 1 - x_lo, core].astype(F32) + co_r[k, 1 - x_lo].astype(F32)
            ).astype(BF16)
            xc[k].start()

    def own(k, q):
        r = pl.ds(16 * q, 16)
        return (
            w[k, x_lo, core, r, :].astype(F32) + co_r[k, x_lo, r, :].astype(F32)
            + xl_r[k, r, :].astype(F32)
        )

    def z_send(k):
        for side in range(2):
            if k < 8 or side == 0:
                xc[(k if side == 0 else -k) % Z].wait_recv()
        for q in range(2):
            for side in range(2):
                if k == 8 and q != side:
                    continue
                kk = (k if side == 0 else -k) % Z
                val = own(kk, q)
                for src, to in HOPS.items():
                    if to == k and (side, src, q) in zc:
                        zc[side, src, q].wait_recv()
                        val = val + zrv[side][src - 1, q].astype(F32)
                zs[kk, q] = val.astype(BF16)
                zc[side, k, q].start()

    w_part(8)
    w_part(7, -7)
    terms(14, 2)
    for u in (1, 0):
        for side in range(2):
            i[side, 1, u].start()
    x_send(8)
    x_send(7, -7)
    w_part(5, -5)
    w_part(4, -4)
    x_send(5, -5)
    w_part(6, -6)
    x_send(4, -4)
    w_part(2, -2)
    x_send(6, -6)
    z_send(8)
    z_send(7)
    w_part(1, -1)
    x_send(2, -2)
    i_step(1)
    w_part(3, -3)
    x_send(1, -1)
    i_step(2)
    z_send(5)
    w_part(0)
    x_send(3, -3)
    z_send(4)
    x_send(0)
    z_send(6)
    i_step(3)
    z_send(2)
    z_send(1)
    i_step(4)
    z_send(3)
    i_step(5)
    i_step(6)
    i_step(7)

    xc[0].wait_recv()
    for q in range(2):
        val = own(0, q)
        for k in (1, 2, 3):
            for side in range(2):
                zc[side, k, q].wait_recv()
                val = val + zrv[side][k - 1, q].astype(F32)
        grad[pl.ds(16 * q, 16), :] = val
    i_step(8)
    ix.wait_recv()
    ig[...] = (
        term[rows(0), :].astype(F32) + ir_r[3, 0].astype(F32) + ir_l[3, 0].astype(F32)
        + xh_r[...].astype(F32)
    ).astype(BF16)

    for cp in [xa, *xb.values(), ix, *xc, *g.values(), *i.values(), *cos, *zc.values()]:
        cp.wait_send()
    for st in upg_st:
        st.wait()


def finish(ig_in, upg_in, grad_in, m1_in, m2_in, ig, upg, m1, m2, upd):
    grad = grad_in[...] * (1.0 / math.sqrt(32768))
    first = 0.9 * m1_in[...].astype(F32) + 0.1 * grad
    second = 0.95 * m2_in[...].astype(F32) + 0.05 * grad * grad
    upd[...] = first / (jnp.sqrt(second) + 1e-8)
    m1[...] = first.astype(BF16)
    m2[...] = second.astype(BF16)
    ig[...] = ig_in[...]
    upg[...] = upg_in[...]


def local(tokens, gate_weight, up_act, cotangent, moment1, moment2):
    dw, hid = gate_weight.shape
    any_spec = pl.BlockSpec(memory_space=pl.ANY)
    vm_spec = pl.BlockSpec(memory_space=pltpu.VMEM)
    vm = pltpu.VMEM
    dma = pltpu.SemaphoreType.DMA
    upg, ig, grad = pl.pallas_call(
        kernel,
        out_shape=(
            jax.ShapeDtypeStruct((16, BLK, hid), BF16),
            jax.ShapeDtypeStruct((BLK, dw), BF16),
            jax.ShapeDtypeStruct((BLK, hid), F32),
        ),
        in_specs=[any_spec] * 4,
        out_specs=(any_spec, vm_spec, vm_spec),
        scratch_shapes=[
            vm((512, dw), BF16),
            vm((dw, hid), BF16),
            vm((512, hid), BF16),
            vm((512, hid), BF16),
            vm((512, hid), BF16),
            vm((512, hid), BF16),
            vm((512, dw), BF16),
            vm((4, 2, BLK, dw), BF16),
            vm((4, 2, BLK, dw), BF16),
            vm((BLK, dw), BF16),
            vm((BLK, dw), BF16),
            vm((Z, 2, 2, BLK, hid), BF16),
            vm((Z, 2, BLK, hid), BF16),
            vm((Z, 2, 16, hid), BF16),
            vm((8, 2, 16, hid), BF16),
            vm((8, 2, 16, hid), BF16),
            vm((Z, BLK, hid), BF16),
            vm((Z, BLK, hid), BF16),
            dma((2,)), dma((16,)), dma((16,)), dma((16,)),
            dma((2, 4, 3)), dma((2, 4, 3)), dma((9,)), dma((9,)), dma, dma, dma((Z,)), dma((Z,)),
            dma((Z,)), dma((Z,)), dma((2, 8, 2)), dma((2, 8, 2)),
            dma((2, 4, 2)), dma((2, 4, 2)),
        ],
        compiler_params=pltpu.CompilerParams(collective_id=0, has_side_effects=True),
    )(tokens, gate_weight, up_act.reshape(16, BLK, hid), cotangent.reshape(16, BLK, hid))
    return pl.pallas_call(
        finish,
        out_shape=(
            jax.ShapeDtypeStruct((BLK, dw), BF16),
            jax.ShapeDtypeStruct((512, hid), BF16),
            jax.ShapeDtypeStruct((BLK, hid), BF16),
            jax.ShapeDtypeStruct((BLK, hid), BF16),
            jax.ShapeDtypeStruct((BLK, hid), F32),
        ),
        in_specs=[vm_spec] * 5,
        out_specs=(vm_spec,) * 5,
    )(ig, upg.reshape(512, hid), grad, moment1, moment2)


def solution(mesh):
    rows, cols, both = P(("dp", "tensor"), None), P(None, "tensor"), P("dp", "tensor")
    return jax.shard_map(
        local,
        mesh=mesh,
        in_specs=(rows, cols, both, both, both, both),
        out_specs=(rows, both, both, both, both),
        check_vma=False,
    )
```
